32 devices in a mesh: groups: 2 (over y), expert: 4 (over z), tensor: 4 (over x, core).
Axes of the slice: x: 2, y: 2, z: 4, core: 2. Of those that a mesh axis runs over, the one named last changes fastest.
Arguments:
- kv_prefill: bfloat16 [32, 512, 2, 1024], P('groups', 'expert', None, 'tensor'), parts along dimension 0, may hold values from -8 to 8
- slot_of: int32 [32], P('groups'), parts along dimension 0, may hold values from 0 to 15, as said below
- lengths: int32 [32], P('groups'), parts along dimension 0, may hold values from 2 to 512
- query: bfloat16 [32, 4096], P(('groups', 'expert'), 'tensor'), parts along dimension 0, may hold values from -100 to 100
- new_kv: bfloat16 [32, 2, 1024], P(('groups', 'expert'), None, 'tensor'), parts along dimension 0, may hold values from -6 to 6
- wo: bfloat16 [4096, 4096], P('tensor', 'expert'), may hold values from -0.09375 to 0.09375
- resid: bfloat16 [32, 4096], P('groups', 'expert'), parts along dimension 0, may hold values from -60 to 60
- norm_gain: bfloat16 [4096], P('expert'), may hold values from 0.25 to 1.75
- expert_ids: int32 [32, 2], P('groups'), parts along dimension 0, may hold values from 0 to 3, all different within a row; in each aligned block of 16 rows (0 to 15, 16 to 31, ...) at most 12 rows name the same one
- gate_logits: float32 [32, 2], P('groups'), parts along dimension 0, may hold values from -6 to 6
- gate_weight_slabs: bfloat16 [4, 4096, 8192], P('expert', None, 'tensor'), may hold values from -0.09375 to 0.09375
- w_up: bfloat16 [4, 4096, 8192], P('expert', None, 'tensor'), may hold values from -0.09375 to 0.09375
- w_down: bfloat16 [4, 8192, 4096], P('expert', 'tensor'), may hold values from -0.0625 to 0.0625
Outputs:
- attn_out: bfloat16 [32, 4096], P('groups', 'expert'), parts along dimension 0
- moe_out: bfloat16 [32, 4096], P(('groups', 'tensor'), 'expert'), parts along dimension 0
The draws below stay inside these ranges and needn't reach their ends.
There are 2 independent parts, one for each index of `groups`. The reference program is written for one: setup_inputs(seed, part) draws one part's arguments, and reference() takes and returns one part's arrays. A program takes and returns all parts, laid end to end along the dimension named above; an argument that names none is the same for every part. Nothing has to cross between parts.
Inputs may be any that keep to these rules, and one draw needn't show every extreme that they name: `slot_of`: a permutation of 0 to 15. `expert_ids`: each expert is named by at most 12 tokens, one of them by exactly 12; no token names an expert twice.
All inputs are finite; a program needn't handle non-finite values.
Results may differ from the reference program's by a relative error of at most 0.023.
Values may be sent and summed in bfloat16 or wider, within the bound.
A program may use at most 128 MiB of HBM per device.

```python
import math
import jax
import jax.numpy as jnp
import numpy as np
from jax import lax

D = 4096
HEADS = 32
KVH = 8
HD = 128
FF = 8192
EXPERTS = 4
TOPK = 2
L = 512
B = 16
SUB = 1
CAP = 12


def slot_order(key):
    return jax.random.permutation(jax.random.fold_in(key, 11), B).astype(jnp.int32)


def draw_slot_of(key, part):
    return slot_order(key)


def draw_kv_prefill(key, part):
    shape_all = (B, L, 2, KVH * HD)
    drawn = jnp.clip(jax.random.normal(jax.random.fold_in(key, 21), shape_all, jnp.float32), -6.0, 6.0)
    return drawn.astype(jnp.bfloat16)


def draw_query(key, part):
    shape_all = (B, HEADS * HD)
    drawn = jnp.clip(jax.random.normal(jax.random.fold_in(key, 41), shape_all, jnp.float32), -6.0, 6.0)
    return drawn.astype(jnp.bfloat16)


def draw_resid(key, part):
    column = jnp.arange(D, dtype=jnp.float32) / D
    base_rows = jnp.clip(jax.random.normal(jax.random.fold_in(key, 53), (B, D), jnp.float32), -6.0, 6.0)
    column_scale = 0.3 * jnp.power(10.0, column)
    row_scale = jnp.exp(jax.random.uniform(jax.random.fold_in(key, 51), (B, 1), jnp.float32, math.log(0.3), math.log(3.0)))
    return (base_rows * row_scale * column_scale[None, :]).astype(jnp.bfloat16)


def place_ends(values, own_key, least, high):
    index_at = [jax.random.randint(jax.random.fold_in(own_key, axis), (), 0, length) for axis, length in enumerate(values.shape)]
    main_axis = values.shape.index(max(values.shape))
    next_to = index_at[:main_axis] + [(index_at[main_axis] + 1) % values.shape[main_axis]] + index_at[main_axis + 1:]
    return values.at[tuple(index_at)].set(least).at[tuple(next_to)].set(high)


def shard_levels(stream_key, shape, cuts, low, high):
    def one(position, parts):
        steps = jax.random.uniform(jax.random.fold_in(jax.random.fold_in(stream_key, 6), position), (parts,), jnp.float32, low / len(cuts), high / len(cuts))
        return jnp.repeat(jnp.exp(steps), shape[position] // parts).reshape((-1,) + (1,) * (len(shape) - position - 1))

    level = one(*cuts[0])
    for cut in cuts[1:]:
        level = level * one(*cut)
    return level


def assign_block(own_key, own, number, rows, amount, top, bound, lean):
    sequence = jax.random.permutation(own_key, amount)
    heavy_load, usual = portions_of(amount, rows * top, bound, lean, True), portions_of(amount, rows * top, bound, lean, False)
    places = jnp.arange(amount)

    def named(tallies, rotation):
        used = int((tallies > 0).sum())
        fixed = max(1, used // 4)
        moved = fixed + (places - fixed + rotation * (used - fixed)) % max(1, amount - fixed)
        return jnp.zeros((amount,), jnp.int32).at[sequence[jnp.where(places < fixed, places, moved)]].set(jnp.asarray(tallies, jnp.int32))

    tallies = jnp.where(number % 4 == 0, named(heavy_load, number // 4), named(usual, number - number // 4 - 1))
    mixed = jax.random.permutation(jax.random.fold_in(own, 3), amount)
    giver, receiver = mixed[0:amount // 2 * 2:2], mixed[1:amount // 2 * 2:2]
    room = jnp.minimum(tallies[giver] - 1, bound - tallies[receiver]) // 2
    room = jnp.where((giver == sequence[0]) | (receiver == sequence[0]) | (tallies[receiver] == 0), 0, jnp.maximum(room, 0))
    moved = jax.random.randint(jax.random.fold_in(own, 4), (amount // 2,), 0, 1 << 20) % (room + 1)
    tallies = tallies.at[giver].add(-moved).at[receiver].add(moved)
    items = jnp.searchsorted(jnp.cumsum(tallies), jnp.arange(rows * top), side="right").astype(jnp.int32)
    grid = items.reshape(top, rows).T
    grid = grid[jax.random.permutation(jax.random.fold_in(own, 1), rows)]
    rotation = jax.random.randint(jax.random.fold_in(own, 2), (rows, 1), 0, top)
    return jnp.take_along_axis(grid, (jnp.arange(top)[None, :] + rotation) % top, axis=1)


def portions_of(count, total, limit, skew, full):
    weights = [(1 << 20) // math.isqrt(grade ** skew) + 1 for grade in range(1, count + 1)]
    largest = limit if full else min(limit, max(-(-total // count), total * weights[0] // sum(weights)))
    least = 1 if total - largest >= count - 1 else 0
    holding, spare = [largest] + [least] * (count - 1), total - largest - least * (count - 1)
    while spare > 0:
        movable = [i for i in range(1, count) if holding[i] < largest] or [i for i in range(1, count) if holding[i] < limit]
        whole, remaining = sum([weights[i] for i in movable]), spare
        for i in movable:
            more = min(limit - holding[i], max(1, remaining * weights[i] // whole), spare)
            holding[i] = holding[i] + more
            spare = spare - more
    return np.array(holding)


def scatter_about(own_key, extent, spread, most, cuts=(), kind=jnp.bfloat16):
    loudness = shard_levels(own_key, extent, cuts, -0.22, 0.18) if cuts else 1.0
    values = jax.random.normal(own_key, extent, jnp.float32) * spread * loudness
    return jnp.minimum(jnp.maximum(values, -most), most).astype(kind)


def setup_inputs(seed: int = 0, part: int = 0) -> dict:
    key_list = jax.random.split(jax.random.key(seed), 14)
    own_keys = jax.random.split(jax.random.fold_in(key_list[13], part), 14)
    kv_prefill = draw_kv_prefill(jax.random.fold_in(jax.random.fold_in(key_list[13], part), 71), part)
    slot_of = draw_slot_of(jax.random.fold_in(jax.random.fold_in(key_list[13], part), 71), part)
    lengths = place_ends(jax.random.randint(own_keys[2], (B,), 2, L + 1), jax.random.fold_in(own_keys[2], 1), 2, L).astype(jnp.int32)
    query = draw_query(jax.random.fold_in(jax.random.fold_in(key_list[13], part), 71), part)
    new_kv = scatter_about(own_keys[4], (B, 2, KVH * HD), 1.0, 6.0, ((0, 4), (2, 4)))
    wo = scatter_about(key_list[5], (HEADS * HD, D), (HEADS * HD) ** -0.5, 0.09375, ((0, 4), (1, 4)))
    resid = draw_resid(jax.random.fold_in(jax.random.fold_in(key_list[13], part), 71), part)
    norm_gain = jnp.clip(1.0 + 0.15 * jax.random.normal(key_list[7], (D,), jnp.float32), 0.25, 1.75).astype(jnp.bfloat16)
    expert_ids_keys = jax.random.split(jax.random.fold_in(own_keys[8], 1), B // B)
    expert_ids_turns = jax.random.permutation(jax.random.fold_in(own_keys[8], 3), B // B)
    expert_ids = jax.vmap(lambda own, number: assign_block(jax.random.fold_in(own_keys[8], 2), own, number, B, EXPERTS, TOPK, CAP, 2))(expert_ids_keys, expert_ids_turns).reshape((B, TOPK))
    gate_logits = scatter_about(own_keys[9], (B, TOPK), 1.5, 6.0, (), jnp.float32)
    gate_weight_slabs = scatter_about(key_list[10], (EXPERTS * SUB, D, FF // SUB), D ** -0.5, 0.09375, ((0, 4), (2, 4)))
    w_up = scatter_about(key_list[11], (EXPERTS * SUB, D, FF // SUB), D ** -0.5, 0.09375, ((0, 4), (2, 4)))
    w_down = scatter_about(key_list[12], (EXPERTS * SUB, FF // SUB, D), FF ** -0.5, 0.0625, ((0, 4), (1, 4)))
    return {"kv_prefill": kv_prefill, "slot_of": slot_of, "lengths": lengths, "query": query, "new_kv": new_kv, "wo": wo, "resid": resid, "norm_gain": norm_gain, "expert_ids": expert_ids, "gate_logits": gate_logits, "gate_weight_slabs": gate_weight_slabs, "w_up": w_up, "w_down": w_down}


EPSILON = 1e-05

def reference(kv_prefill, slot_of, lengths, query, new_kv, wo, resid, norm_gain, expert_ids, gate_logits, gate_weight_slabs, w_up, w_down):
    group_size = HEADS // KVH
    logit_scale_factor = 1.0 / math.sqrt(HD)
    cached = jnp.take(kv_prefill, slot_of, axis=0)
    key_rows = cached[:, :, 0, :].reshape(B, L, KVH, HD).astype(jnp.float32)
    value_rows = cached[:, :, 1, :].reshape(B, L, KVH, HD).astype(jnp.float32)
    query_vectors = query.reshape(B, KVH, group_size, HD).astype(jnp.float32)
    scores = jnp.einsum('bkqd,bpkd->bkqp', query_vectors, key_rows) * logit_scale_factor
    live_mask = jnp.arange(L, dtype=jnp.int32)[None, :] < lengths[:, None]
    live_mask = live_mask[:, None, None, :]
    scores = jnp.where(live_mask, scores, -1e+30)
    cache_peak = lax.optimization_barrier(jnp.max(scores, axis=-1))
    exp_weights = jnp.where(live_mask, jnp.exp(scores - cache_peak[..., None]), 0.0)
    cache_total = lax.optimization_barrier(jnp.sum(exp_weights, axis=-1))
    rounded = lax.optimization_barrier(exp_weights.astype(jnp.bfloat16)).astype(jnp.float32)
    summed = jnp.einsum('bkqp,bpkd->bkqd', rounded, value_rows)
    fresh_key_rows = new_kv[:, 0, :].reshape(B, KVH, HD).astype(jnp.float32)
    new_values = new_kv[:, 1, :].reshape(B, KVH, HD).astype(jnp.float32)
    self_score_value = jnp.einsum('utfa,uta->utf', query_vectors, fresh_key_rows) * logit_scale_factor
    peak_value = jnp.maximum(cache_peak, self_score_value)
    old_part = jnp.exp(cache_peak - peak_value)
    own_part = jnp.exp(self_score_value - peak_value)
    numerator = summed * old_part[..., None] + own_part[..., None] * new_values[:, :, None, :]
    denominator = cache_total * old_part + own_part
    context = (numerator / denominator[..., None]).reshape(B, HEADS * HD).astype(jnp.bfloat16)
    attn_out = jnp.dot(context, wo, preferred_element_type=jnp.float32).astype(jnp.bfloat16)
    hidden_activation = resid.astype(jnp.float32) + attn_out.astype(jnp.float32)
    mean_square = lax.optimization_barrier(jnp.mean(hidden_activation * hidden_activation, axis=1, keepdims=True))
    normed = (hidden_activation * lax.rsqrt(mean_square + EPSILON) * norm_gain.astype(jnp.float32)[None, :]).astype(jnp.bfloat16)
    first_share = 1.0 / (1.0 + jnp.exp(gate_logits[:, 1] - gate_logits[:, 0]))
    shares = jnp.stack([first_share, 1.0 - first_share], axis=1)
    chosen = expert_ids[:, :, None] == jnp.arange(EXPERTS, dtype=jnp.int32)[None, None, :]
    mixture = lax.optimization_barrier(jnp.sum(jnp.where(chosen, shares[:, :, None], 0.0), axis=1))

    def expert_term(expert_index):
        slab_begin_offset = expert_index * SUB
        gate_slab = lax.dynamic_slice_in_dim(gate_weight_slabs, slab_begin_offset, SUB, 0)
        gate_slab = jnp.moveaxis(gate_slab, 0, 1).reshape(D, FF)
        up_slab = lax.dynamic_slice_in_dim(w_up, slab_begin_offset, SUB, 0)
        up_slab = jnp.moveaxis(up_slab, 0, 1).reshape(D, FF)
        down_slab = lax.dynamic_slice_in_dim(w_down, slab_begin_offset, SUB, 0).reshape(FF, D)
        gate_sum = jnp.dot(normed, gate_slab, preferred_element_type=jnp.float32)
        up_sum = jnp.dot(normed, up_slab, preferred_element_type=jnp.float32)
        activated = (jax.nn.silu(gate_sum) * up_sum).astype(jnp.bfloat16)
        weight_column = lax.dynamic_index_in_dim(mixture, expert_index, 1, keepdims=True)
        return jnp.dot(activated, down_slab, preferred_element_type=jnp.float32) * weight_column
    contributions = lax.map(expert_term, jnp.arange(EXPERTS, dtype=jnp.int32))
    moe_out = lax.optimization_barrier(jnp.sum(contributions, axis=0)).astype(jnp.bfloat16)
    return (attn_out, moe_out)
```

```python
import functools
import math

import jax
import jax.numpy as jnp
from jax import lax
from jax.experimental import pallas as pl
from jax.experimental.pallas import tpu as pltpu
from jax.sharding import PartitionSpec as P

D = 4096
HEADS = 32
KVH = 8
HD = 128
EXPERTS = 4


EPSILON = 1e-05
MASKED = -1e30


def cache_partial(query_vectors, key_rows, value_rows, live_mask, logit_scale_factor):
    scores = (
        jnp.einsum("rkqd,rpkd->rkqp", query_vectors, key_rows, preferred_element_type=jnp.float32)
        * logit_scale_factor
    )
    mask_rows = live_mask[:, None, None, :]
    scores = jnp.where(mask_rows, scores, MASKED)
    peak_value = jnp.max(scores, axis=-1)
    exp_weights = jnp.where(mask_rows, jnp.exp(scores - peak_value[..., None]), 0.0)
    denominator = jnp.sum(exp_weights, axis=-1)
    summed = jnp.einsum(
        "rkqp,rpkd->rkqd",
        exp_weights.astype(jnp.bfloat16),
        value_rows,
        preferred_element_type=jnp.float32,
    )
    return (peak_value, denominator, summed)


def combine(earlier, latter):
    peak_value = jnp.maximum(earlier[0], latter[0])
    weight_left = jnp.exp(earlier[0] - peak_value)
    weight_right = jnp.exp(latter[0] - peak_value)
    denominator = earlier[1] * weight_left + latter[1] * weight_right
    summed = earlier[2] * weight_left[..., None] + latter[2] * weight_right[..., None]
    return (peak_value, denominator, summed)


def finish(state, query_vectors, new_rows, logit_scale_factor):
    row_count, kv_local, group_size, head_size = query_vectors.shape
    fresh_key_rows = new_rows[:, 0, :].reshape(row_count, kv_local, head_size)
    new_values = new_rows[:, 1, :].reshape(row_count, kv_local, 1, head_size).astype(jnp.float32)
    self_score_value = (
        jnp.einsum(
            "rkqd,rkd->rkq", query_vectors, fresh_key_rows, preferred_element_type=jnp.float32
        )
        * logit_scale_factor
    )
    own_state = (
        self_score_value,
        jnp.ones_like(self_score_value),
        jnp.broadcast_to(new_values, query_vectors.shape),
    )
    peak_value, denominator, summed = combine(state, own_state)
    return (
        (summed / denominator[..., None])
        .reshape(row_count, kv_local * group_size * head_size)
        .astype(jnp.bfloat16)
    )


def shards(
    kv_prefill,
    slot_of,
    lengths,
    query,
    new_kv,
    wo,
    resid,
    norm_gain,
    expert_ids,
    gate_logits,
    gate_weight_slabs,
    w_up,
    w_down,
):
    axis_count = lax.axis_size("expert")
    my_index = lax.axis_index("expert")
    kv_local = kv_prefill.shape[3] // HD
    group_size = HEADS // KVH
    logit_scale_factor = 1.0 / math.sqrt(HD)
    seq_count = query.shape[0]
    total_rows = lengths.shape[0]
    ordered = jnp.take(kv_prefill, slot_of, axis=0)
    own_cache = lax.all_to_all(ordered, "expert", split_axis=0, concat_axis=1, tiled=True)
    positions = own_cache.shape[1]
    key_rows = own_cache[:, :, 0, :].reshape(seq_count, positions, kv_local, HD)
    value_rows = own_cache[:, :, 1, :].reshape(seq_count, positions, kv_local, HD)
    own_lengths = lax.dynamic_slice_in_dim(lengths, my_index * seq_count, seq_count)
    live_mask = jnp.arange(positions, dtype=jnp.int32)[None, :] < own_lengths[:, None]
    query_vectors = query.reshape(seq_count, kv_local, group_size, HD)
    state = cache_partial(query_vectors, key_rows, value_rows, live_mask, logit_scale_factor)
    context = finish(state, query_vectors, new_kv, logit_scale_factor)
    partial_out = jnp.dot(
        lax.all_gather(context, "expert", axis=0, tiled=True),
        wo,
        preferred_element_type=jnp.float32,
    )
    attention = lax.psum(partial_out.astype(jnp.bfloat16), "tensor")
    hidden_activation = resid.astype(jnp.float32) + attention.astype(jnp.float32)
    squares = lax.psum(jnp.sum(hidden_activation * hidden_activation, axis=1), "expert")
    normed = (
        hidden_activation
        * lax.rsqrt(squares / D + EPSILON)[:, None]
        * norm_gain.astype(jnp.float32)[None, :]
    ).astype(jnp.bfloat16)
    first_share = 1.0 / (1.0 + jnp.exp(gate_logits[:, 1] - gate_logits[:, 0]))
    shares = jnp.stack([first_share, 1.0 - first_share], axis=1)
    sharing = axis_count // EXPERTS
    my_expert = my_index // sharing
    mine_mask = expert_ids == my_expert
    mix_mine = jnp.sum(jnp.where(mine_mask, shares, 0.0), axis=1)
    gate_slab = gate_weight_slabs[0]
    up_slab = w_up[0]
    down_slab = w_down[0]
    capacity = 3 * total_rows // 4
    expert_range = jnp.arange(EXPERTS, dtype=jnp.int32)
    picked = jnp.any(expert_ids[:, :, None] == expert_range[None, None, :], axis=1).astype(
        jnp.int32
    )
    rank_of = jnp.cumsum(picked, axis=0) - 1
    slot_range = jnp.arange(capacity, dtype=jnp.int32)
    slot_hits = (picked[:, :, None] > 0) & (rank_of[:, :, None] == slot_range[None, None, :])
    token_range = jnp.arange(total_rows, dtype=jnp.int32)[:, None, None]
    token_table = jnp.sum(jnp.where(slot_hits, token_range, 0), axis=0)
    token_table = token_table + jnp.where(jnp.any(slot_hits, axis=0), 0, total_rows)
    padded_rows = jnp.concatenate([normed, jnp.zeros((1, normed.shape[1]), jnp.bfloat16)], axis=0)
    blocks = jnp.take(padded_rows, token_table, axis=0)
    outgoing = jnp.repeat(blocks, sharing, axis=0)
    arrived = lax.all_to_all(outgoing, "expert", split_axis=0, concat_axis=2, tiled=True)[0]
    gate_sum = jnp.dot(arrived, gate_slab, preferred_element_type=jnp.float32)
    up_sum = jnp.dot(arrived, up_slab, preferred_element_type=jnp.float32)
    activated = (jax.nn.silu(gate_sum) * up_sum).astype(jnp.bfloat16)
    produced = jnp.dot(activated, down_slab, preferred_element_type=jnp.float32)
    own_picked = jnp.any(mine_mask, axis=1)
    own_rank = jnp.sum(jnp.where(expert_range[None, :] == my_expert, rank_of, 0), axis=1)
    slot_index = jnp.where(own_picked, own_rank, capacity)
    padded_out = jnp.concatenate([produced, jnp.zeros((1, produced.shape[1]), jnp.float32)], axis=0)
    contrib = jnp.take(padded_out, slot_index, axis=0) * mix_mine[:, None]
    column_part = lax.psum_scatter(
        contrib.astype(jnp.bfloat16), "expert", scatter_dimension=1, tiled=True
    )
    summed_out = lax.psum_scatter(column_part, "tensor", scatter_dimension=0, tiled=True).astype(
        jnp.float32
    )
    moe_out = summed_out.astype(jnp.bfloat16)
    return (attention, moe_out)


MESH = pl.DeviceIdType.MESH


def remote(source, target, sems, index, where):
    return pltpu.make_async_remote_copy(
        src_ref=source,
        dst_ref=target,
        send_sem=sems.at[0, index],
        recv_sem=sems.at[1, index],
        device_id=where,
        device_id_type=MESH,
    )


def fused_kernel(
    experts_n,
    tensor_n,
    slot_ref,
    len_ref,
    q_ref,
    new_ref,
    resid_ref,
    gain_ref,
    ids_ref,
    logits_ref,
    kv_hbm,
    wo_hbm,
    wg_hbm,
    wu_hbm,
    wd_hbm,
    attn_ref,
    moe_ref,
    kv_v,
    wo_v,
    wg_v,
    wu_v,
    wd_v,
    qall,
    head_rows,
    pacc,
    pstat,
    abuf,
    hbuf,
    ssq,
    gacc,
    uacc,
    act,
    sbuf,
    rbuf,
    load_sem,
    wg_sem,
    wu_sem,
    wd_sem,
    q_sem,
    pacc_sem,
    pstat_sem,
    a_sem,
    h_sem,
    ssq_sem,
    r_sem,
):
    e = lax.axis_index("expert")
    t = lax.axis_index("tensor")
    own_seqs = q_ref.shape[0]
    seqs = own_seqs * experts_n
    heads = q_ref.shape[1] // HD
    kv_local = new_ref.shape[2] // HD
    group_size = heads // kv_local
    keys2 = kv_v.shape[1]
    positions = keys2 // 2
    cols = wo_v.shape[1]
    scale = 1.0 / math.sqrt(HD)
    f32 = jnp.float32
    bf16 = jnp.bfloat16

    kv_load = pltpu.make_async_copy(kv_hbm, kv_v, load_sem.at[0])
    kv_load.start()
    wo_load = pltpu.make_async_copy(wo_hbm, wo_v, load_sem.at[1])
    wo_load.start()

    def column_block(step, sign):
        return lax.rem(e + sign * step + experts_n, experts_n) * cols

    gate_loads, up_loads, down_loads = [], [], []
    for step in range(experts_n):
        rows = pl.ds(pl.multiple_of(column_block(step, -1), 128), cols)
        for hbm, vmem, sem, loads in (
            (wg_hbm, wg_v, wg_sem, gate_loads),
            (wu_hbm, wu_v, wu_sem, up_loads),
        ):
            load = pltpu.make_async_copy(hbm.at[0, rows, :], vmem.at[rows, :], sem.at[step])
            load.start()
            loads.append(load)
    down_order = list(range(1, experts_n)) + [0]
    for step in down_order:
        block = pl.ds(pl.multiple_of(column_block(step, 1), 128), cols)
        load = pltpu.make_async_copy(
            wd_hbm.at[0, :, block], wd_v.at[:, block], wd_sem.at[step]
        )
        load.start()
        down_loads.append(load)

    barrier = pltpu.get_barrier_semaphore()
    for k in range(1, experts_n * tensor_n):
        where = {
            "expert": lax.rem(e + k // tensor_n, experts_n),
            "tensor": lax.rem(t + k % tensor_n, tensor_n),
        }
        pl.semaphore_signal(barrier, inc=1, device_id=where, device_id_type=MESH)
    pl.semaphore_wait(barrier, experts_n * tensor_n - 1)

    sends = []
    q_copies = []
    for step in range(1, experts_n):
        copy = remote(
            q_ref, qall.at[e], q_sem, step, {"expert": lax.rem(e + step, experts_n)}
        )
        copy.start()
        q_copies.append(copy)
    qall[e] = q_ref[...]
    kv_load.wait()
    for copy in q_copies:
        copy.wait_recv()
    for owner in range(experts_n):
        block = qall[owner].astype(f32)
        for h in range(heads):
            head_rows[pl.ds(owner * own_seqs * heads + h, own_seqs, stride=heads), :] = block[
                :, h * HD : (h + 1) * HD
            ]

    row_of = lax.broadcasted_iota(jnp.int32, (heads, HD), 0)
    column = lax.broadcasted_iota(jnp.int32, (heads, keys2), 1)
    is_key = lax.rem(column, 2) == 0
    position = e * positions + lax.div(column, 2)

    def by_group(pieces):
        picked = pieces[0]
        for g in range(1, kv_local):
            picked = jnp.where(row_of >= g * group_size, pieces[g], picked)
        return picked

    score_list, live_list, own_list, value_list = [], [], [], []
    for b in range(seqs):
        q_rows = head_rows[b * heads : (b + 1) * heads, :]
        spread = jnp.concatenate(
            [
                jnp.where(lax.div(row_of, group_size) == g, q_rows, 0.0)
                for g in range(kv_local)
            ],
            axis=1,
        ).astype(bf16)
        cache = kv_v[slot_ref[b]]
        raw = lax.dot_general(
            spread, cache, (((1,), (1,)), ((), ())), preferred_element_type=f32
        )
        live = is_key & (position < len_ref[b])
        score_list.append(jnp.where(live, raw * scale, MASKED))
        live_list.append(jnp.where(live, 1.0, 0.0))
        fresh = new_ref[b % own_seqs].astype(f32)
        fresh_keys = by_group([fresh[0:1, g * HD : (g + 1) * HD] for g in range(kv_local)])
        own = jnp.sum(q_rows * fresh_keys, axis=1, keepdims=True) * scale
        own_list.append(jnp.where(e == b // own_seqs, own, MASKED))
        value_list.append(
            jnp.broadcast_to(
                by_group([fresh[1:2, g * HD : (g + 1) * HD] for g in range(kv_local)]),
                (heads, HD),
            )
        )
    scores = jnp.concatenate(score_list, axis=0)
    live = jnp.concatenate(live_list, axis=0)
    own = jnp.concatenate(own_list, axis=0)
    peak = jnp.maximum(jnp.max(scores, axis=1, keepdims=True), own)
    weights = jnp.exp(scores - peak) * live
    own_weight = jnp.where(own > 0.5 * MASKED, jnp.exp(own - peak), 0.0)
    total = jnp.sum(weights, axis=1, keepdims=True) + own_weight
    shifted = pltpu.roll(weights, 1, 1).astype(bf16)
    for b in range(seqs):
        out = jnp.dot(
            shifted[b * heads : (b + 1) * heads, :],
            kv_v[slot_ref[b]],
            preferred_element_type=f32,
        )
        picked = by_group([out[:, g * HD : (g + 1) * HD] for g in range(kv_local)])
        picked = picked + own_weight[b * heads : (b + 1) * heads] * value_list[b]
        head_rows[b * heads : (b + 1) * heads, :] = picked
    pacc[0] = head_rows[...].astype(bf16)
    lane = lax.broadcasted_iota(jnp.int32, (seqs * heads, HD), 1)
    stats = jnp.where(lane == 0, peak, jnp.where(lane == 1, total, 0.0))
    pstat[0] = stats.T[0:8, :]

    p_copies = []
    for step in range(1, experts_n):
        where = {"expert": lax.rem(e + step, experts_n)}
        for buffer, sem in ((pstat, pstat_sem), (pacc, pacc_sem)):
            copy = remote(buffer.at[0], buffer.at[step], sem, step, where)
            copy.start()
            p_copies.append(copy)

    logits = logits_ref[...]
    first_share = 1.0 / (1.0 + jnp.exp(logits[:, 1:2] - logits[:, 0:1]))
    ids = ids_ref[...]
    mix = jnp.where(ids[:, 0:1] == e, first_share, 0.0) + jnp.where(
        ids[:, 1:2] == e, 1.0 - first_share, 0.0
    )

    wo_load.wait()
    for copy in p_copies:
        copy.wait_recv()
    peaks = [pstat[j][0:1, :] for j in range(experts_n)]
    top = functools.reduce(jnp.maximum, peaks)
    factors = [jnp.exp(p - top) for p in peaks]
    whole = sum(f * pstat[j][1:2, :] for j, f in enumerate(factors))
    row8 = lax.broadcasted_iota(jnp.int32, (8, seqs * heads), 0)
    stacked = jnp.zeros((8, seqs * heads), f32)
    for j, f in enumerate(factors):
        stacked = jnp.where(row8 == j, f / whole, stacked)
    turned = stacked.T
    context = sum(pacc[j].astype(f32) * turned[:, j : j + 1] for j in range(experts_n))
    head_rows[...] = context
    context = jnp.concatenate(
        [head_rows[pl.ds(h, seqs, stride=heads), :] for h in range(heads)], axis=1
    ).astype(bf16)
    abuf[t] = jnp.dot(context, wo_v[...], preferred_element_type=f32).astype(bf16)

    a_copies = []
    for step in range(1, tensor_n):
        copy = remote(
            abuf.at[t], abuf.at[t], a_sem, step, {"tensor": lax.rem(t + step, tensor_n)}
        )
        copy.start()
        a_copies.append(copy)
    for copy in a_copies:
        copy.wait_recv()
    attention = sum(abuf[j].astype(f32) for j in range(tensor_n)).astype(bf16)
    attn_ref[...] = attention
    hidden = resid_ref[...].astype(f32) + attention.astype(f32)
    hbuf[0] = (hidden * gain_ref[...].astype(f32)).astype(bf16)
    ssq[0] = jnp.broadcast_to(jnp.sum(hidden * hidden, axis=1, keepdims=True), ssq.shape[1:])
    h_copies, s_copies = [None], [None]
    for step in range(1, experts_n):
        where = {"expert": lax.rem(e + step, experts_n)}
        copy = remote(hbuf.at[0], hbuf.at[step], h_sem, step, where)
        copy.start()
        h_copies.append(copy)
        copy = remote(ssq.at[0], ssq.at[step], ssq_sem, step, where)
        copy.start()
        s_copies.append(copy)

    hidden_units = wg_v.shape[1]
    width = math.gcd(hidden_units, 512)
    for step in range(experts_n):
        if step:
            h_copies[step].wait_recv()
        gate_loads[step].wait()
        up_loads[step].wait()
        rows = pl.ds(pl.multiple_of(column_block(step, -1), 128), cols)
        tokens = hbuf[step]

        def one(i, carry, rows=rows, tokens=tokens, step=step):
            block = pl.ds(pl.multiple_of(i * width, width), width)
            gate = jnp.dot(tokens, wg_v[rows, block], preferred_element_type=f32)
            up = jnp.dot(tokens, wu_v[rows, block], preferred_element_type=f32)
            if step:
                gate = gate + gacc[:, block]
                up = up + uacc[:, block]
            gacc[:, block] = gate
            uacc[:, block] = up
            return carry

        lax.fori_loop(0, hidden_units // width, one, 0)
    for step in range(1, experts_n):
        s_copies[step].wait_recv()
    squares = sum(ssq[j][:, 0:1] for j in range(experts_n))
    inverse = lax.rsqrt(squares / (cols * experts_n) + EPSILON)
    gate = gacc[...] * inverse
    up = uacc[...] * inverse
    act[...] = (gate / (1.0 + jnp.exp(-gate)) * up).astype(bf16)

    out_rows = seqs // tensor_n
    down_width = math.gcd(cols, 512)
    r_copies = []
    for step, load in zip(down_order, down_loads):
        load.wait()
        start = column_block(step, 1)

        def one_down(i, carry, start=start, step=step):
            offset = pl.multiple_of(i * down_width, down_width)
            block = pl.ds(pl.multiple_of(start + offset, 128), down_width)
            made = jnp.dot(act[...], wd_v[:, block], preferred_element_type=f32) * mix
            for p in range(tensor_n):
                sbuf[step, p, :, pl.ds(offset, down_width)] = made[
                    p * out_rows : (p + 1) * out_rows
                ].astype(bf16)
            return carry

        lax.fori_loop(0, cols // down_width, one_down, 0)
        for turn in range(tensor_n):
            if step == 0 and turn == 0:
                continue
            k = step * tensor_n + turn
            target = lax.rem(t + turn, tensor_n)
            where = {"expert": lax.rem(e + step, experts_n), "tensor": target}
            copy = remote(sbuf.at[step, target], rbuf.at[k], r_sem, k, where)
            copy.start()
            r_copies.append(copy)
    result = sbuf[0, t].astype(f32)
    for copy in r_copies:
        copy.wait_recv()
    for k in range(1, experts_n * tensor_n):
        result = result + rbuf[k].astype(f32)
    moe_ref[...] = result.astype(bf16)
    for copy in (
        q_copies + p_copies + a_copies + h_copies[1:] + s_copies[1:] + r_copies
    ):
        copy.wait_send()


def fused(
    kv_prefill, slot_of, lengths, query, new_kv, wo, resid, norm_gain, expert_ids,
    gate_logits, gate_weight_slabs, w_up, w_down,
):
    experts_n = lax.axis_size("expert")
    tensor_n = lax.axis_size("tensor")
    slots, positions, _, kv_cols = kv_prefill.shape
    own_seqs = query.shape[0]
    seqs = lengths.shape[0]
    cols = resid.shape[1]
    heads = query.shape[1] // HD
    hidden_units = w_down.shape[1]
    out_rows = seqs // tensor_n
    bf16 = jnp.bfloat16
    f32 = jnp.float32
    vmem = pl.BlockSpec(memory_space=pltpu.VMEM)
    smem = pl.BlockSpec(memory_space=pltpu.SMEM)
    hbm = pl.BlockSpec(memory_space=pl.ANY)
    dma = pltpu.SemaphoreType.DMA
    peers = experts_n * tensor_n
    return tuple(
        pl.pallas_call(
            functools.partial(fused_kernel, experts_n, tensor_n),
            out_shape=(
                jax.ShapeDtypeStruct((seqs, cols), bf16),
                jax.ShapeDtypeStruct((out_rows, cols), bf16),
            ),
            in_specs=[smem, smem] + [vmem] * 6 + [hbm] * 5,
            out_specs=(vmem, vmem),
            scratch_shapes=[
                pltpu.VMEM((slots, positions * 2, kv_cols), bf16),
                pltpu.VMEM(wo.shape, bf16),
                pltpu.VMEM(gate_weight_slabs.shape[1:], bf16),
                pltpu.VMEM(w_up.shape[1:], bf16),
                pltpu.VMEM(w_down.shape[1:], bf16),
                pltpu.VMEM((experts_n,) + query.shape, bf16),
                pltpu.VMEM((seqs * heads, HD), f32),
                pltpu.VMEM((experts_n, seqs * heads, HD), bf16),
                pltpu.VMEM((experts_n, 8, seqs * heads), f32),
                pltpu.VMEM((tensor_n, seqs, cols), bf16),
                pltpu.VMEM((experts_n, seqs, cols), bf16),
                pltpu.VMEM((experts_n, seqs, 128), f32),
                pltpu.VMEM((seqs, hidden_units), f32),
                pltpu.VMEM((seqs, hidden_units), f32),
                pltpu.VMEM((seqs, hidden_units), bf16),
                pltpu.VMEM((experts_n, tensor_n, out_rows, cols), bf16),
                pltpu.VMEM((peers, out_rows, cols), bf16),
                dma((2,)),
                dma((experts_n,)),
                dma((experts_n,)),
                dma((experts_n,)),
                dma((2, experts_n)),
                dma((2, experts_n)),
                dma((2, experts_n)),
                dma((2, tensor_n)),
                dma((2, experts_n)),
                dma((2, experts_n)),
                dma((2, peers)),
            ],
            compiler_params=pltpu.CompilerParams(
                collective_id=0, has_side_effects=True, vmem_limit_bytes=60 * 1024 * 1024
            ),
        )(
            slot_of, lengths, query, new_kv, resid, norm_gain.reshape(1, cols), expert_ids,
            gate_logits, kv_prefill.reshape(slots, positions * 2, kv_cols), wo,
            gate_weight_slabs, w_up, w_down,
        )
    )


def layer(*arrays):
    kv_prefill, slot_of, lengths, query = arrays[:4]
    gate_slabs = arrays[10]
    weights = 3 * gate_slabs.size * 2
    rows = lengths.shape[0] * (query.shape[1] // HD)
    if (
        lax.axis_size("expert") == EXPERTS
        and gate_slabs.shape[0] == 1
        and (2 * kv_prefill.shape[1]) % 128 == 0
        and (query.shape[1] // HD) % 8 == 0
        and lengths.shape[0] % 16 == 0
        and rows == 128
        and weights <= 52 * 2**20
    ):
        return fused(*arrays)
    return shards(*arrays)


def solution(mesh):
    return jax.shard_map(
        layer,
        mesh=mesh,
        in_specs=(
            P("groups", "expert", None, "tensor"),
            P("groups"),
            P("groups"),
            P(("groups", "expert"), "tensor"),
            P(("groups", "expert"), None, "tensor"),
            P("tensor", "expert"),
            P("groups", "expert"),
            P("expert"),
            P("groups", None),
            P("groups", None),
            P("expert", None, "tensor"),
            P("expert", None, "tensor"),
            P("expert", "tensor", None),
        ),
        out_specs=(P("groups", "expert"), P(("groups", "tensor"), "expert")),
        check_vma=False,
    )
```

```python
import functools
import math

import jax
import jax.numpy as jnp
from jax import lax
from jax.experimental import pallas as pl
from jax.experimental.pallas import tpu as pltpu
from jax.sharding import PartitionSpec as P

D = 4096
HEADS = 32
KVH = 8
HD = 128
EXPERTS = 4


EPSILON = 1e-05
MASKED = -1e30


def cache_partial(query_vectors, key_rows, value_rows, live_mask, logit_scale_factor):
    scores = (
        jnp.einsum("rkqd,rpkd->rkqp", query_vectors, key_rows, preferred_element_type=jnp.float32)
        * logit_scale_factor
    )
    mask_rows = live_mask[:, None, None, :]
    scores = jnp.where(mask_rows, scores, MASKED)
    peak_value = jnp.max(scores, axis=-1)
    exp_weights = jnp.where(mask_rows, jnp.exp(scores - peak_value[..., None]), 0.0)
    denominator = jnp.sum(exp_weights, axis=-1)
    summed = jnp.einsum(
        "rkqp,rpkd->rkqd",
        exp_weights.astype(jnp.bfloat16),
        value_rows,
        preferred_element_type=jnp.float32,
    )
    return (peak_value, denominator, summed)


def combine(earlier, latter):
    peak_value = jnp.maximum(earlier[0], latter[0])
    weight_left = jnp.exp(earlier[0] - peak_value)
    weight_right = jnp.exp(latter[0] - peak_value)
    denominator = earlier[1] * weight_left + latter[1] * weight_right
    summed = earlier[2] * weight_left[..., None] + latter[2] * weight_right[..., None]
    return (peak_value, denominator, summed)


def finish(state, query_vectors, new_rows, logit_scale_factor):
    row_count, kv_local, group_size, head_size = query_vectors.shape
    fresh_key_rows = new_rows[:, 0, :].reshape(row_count, kv_local, head_size)
    new_values = new_rows[:, 1, :].reshape(row_count, kv_local, 1, head_size).astype(jnp.float32)
    self_score_value = (
        jnp.einsum(
            "rkqd,rkd->rkq", query_vectors, fresh_key_rows, preferred_element_type=jnp.float32
        )
        * logit_scale_factor
    )
    own_state = (
        self_score_value,
        jnp.ones_like(self_score_value),
        jnp.broadcast_to(new_values, query_vectors.shape),
    )
    peak_value, denominator, summed = combine(state, own_state)
    return (
        (summed / denominator[..., None])
        .reshape(row_count, kv_local * group_size * head_size)
        .astype(jnp.bfloat16)
    )


def shards(
    kv_prefill,
    slot_of,
    lengths,
    query,
    new_kv,
    wo,
    resid,
    norm_gain,
    expert_ids,
    gate_logits,
    gate_weight_slabs,
    w_up,
    w_down,
):
    axis_count = lax.axis_size("expert")
    my_index = lax.axis_index("expert")
    kv_local = kv_prefill.shape[3] // HD
    group_size = HEADS // KVH
    logit_scale_factor = 1.0 / math.sqrt(HD)
    seq_count = query.shape[0]
    total_rows = lengths.shape[0]
    ordered = jnp.take(kv_prefill, slot_of, axis=0)
    own_cache = lax.all_to_all(ordered, "expert", split_axis=0, concat_axis=1, tiled=True)
    positions = own_cache.shape[1]
    key_rows = own_cache[:, :, 0, :].reshape(seq_count, positions, kv_local, HD)
    value_rows = own_cache[:, :, 1, :].reshape(seq_count, positions, kv_local, HD)
    own_lengths = lax.dynamic_slice_in_dim(lengths, my_index * seq_count, seq_count)
    live_mask = jnp.arange(positions, dtype=jnp.int32)[None, :] < own_lengths[:, None]
    query_vectors = query.reshape(seq_count, kv_local, group_size, HD)
    state = cache_partial(query_vectors, key_rows, value_rows, live_mask, logit_scale_factor)
    context = finish(state, query_vectors, new_kv, logit_scale_factor)
    partial_out = jnp.dot(
        lax.all_gather(context, "expert", axis=0, tiled=True),
        wo,
        preferred_element_type=jnp.float32,
    )
    attention = lax.psum(partial_out.astype(jnp.bfloat16), "tensor")
    hidden_activation = resid.astype(jnp.float32) + attention.astype(jnp.float32)
    squares = lax.psum(jnp.sum(hidden_activation * hidden_activation, axis=1), "expert")
    normed = (
        hidden_activation
        * lax.rsqrt(squares / D + EPSILON)[:, None]
        * norm_gain.astype(jnp.float32)[None, :]
    ).astype(jnp.bfloat16)
    first_share = 1.0 / (1.0 + jnp.exp(gate_logits[:, 1] - gate_logits[:, 0]))
    shares = jnp.stack([first_share, 1.0 - first_share], axis=1)
    sharing = axis_count // EXPERTS
    my_expert = my_index // sharing
    mine_mask = expert_ids == my_expert
    mix_mine = jnp.sum(jnp.where(mine_mask, shares, 0.0), axis=1)
    gate_slab = gate_weight_slabs[0]
    up_slab = w_up[0]
    down_slab = w_down[0]
    capacity = 3 * total_rows // 4
    expert_range = jnp.arange(EXPERTS, dtype=jnp.int32)
    picked = jnp.any(expert_ids[:, :, None] == expert_range[None, None, :], axis=1).astype(
        jnp.int32
    )
    rank_of = jnp.cumsum(picked, axis=0) - 1
    slot_range = jnp.arange(capacity, dtype=jnp.int32)
    slot_hits = (picked[:, :, None] > 0) & (rank_of[:, :, None] == slot_range[None, None, :])
    token_range = jnp.arange(total_rows, dtype=jnp.int32)[:, None, None]
    token_table = jnp.sum(jnp.where(slot_hits, token_range, 0), axis=0)
    token_table = token_table + jnp.where(jnp.any(slot_hits, axis=0), 0, total_rows)
    padded_rows = jnp.concatenate([normed, jnp.zeros((1, normed.shape[1]), jnp.bfloat16)], axis=0)
    blocks = jnp.take(padded_rows, token_table, axis=0)
    outgoing = jnp.repeat(blocks, sharing, axis=0)
    arrived = lax.all_to_all(outgoing, "expert", split_axis=0, concat_axis=2, tiled=True)[0]
    gate_sum = jnp.dot(arrived, gate_slab, preferred_element_type=jnp.float32)
    up_sum = jnp.dot(arrived, up_slab, preferred_element_type=jnp.float32)
    activated = (jax.nn.silu(gate_sum) * up_sum).astype(jnp.bfloat16)
    produced = jnp.dot(activated, down_slab, preferred_element_type=jnp.float32)
    own_picked = jnp.any(mine_mask, axis=1)
    own_rank = jnp.sum(jnp.where(expert_range[None, :] == my_expert, rank_of, 0), axis=1)
    slot_index = jnp.where(own_picked, own_rank, capacity)
    padded_out = jnp.concatenate([produced, jnp.zeros((1, produced.shape[1]), jnp.float32)], axis=0)
    contrib = jnp.take(padded_out, slot_index, axis=0) * mix_mine[:, None]
    column_part = lax.psum_scatter(
        contrib.astype(jnp.bfloat16), "expert", scatter_dimension=1, tiled=True
    )
    summed_out = lax.psum_scatter(column_part, "tensor", scatter_dimension=0, tiled=True).astype(
        jnp.float32
    )
    moe_out = summed_out.astype(jnp.bfloat16)
    return (attention, moe_out)


MESH = pl.DeviceIdType.MESH


def remote(source, target, sems, index, where):
    return pltpu.make_async_remote_copy(
        src_ref=source,
        dst_ref=target,
        send_sem=sems.at[0, index],
        recv_sem=sems.at[1, index],
        device_id=where,
        device_id_type=MESH,
    )


def fused_kernel(
    experts_n,
    tensor_n,
    slot_ref,
    len_ref,
    q_ref,
    new_ref,
    resid_ref,
    gain_ref,
    ids_ref,
    logits_ref,
    kv_hbm,
    wo_hbm,
    wg_hbm,
    wu_hbm,
    wd_hbm,
    attn_ref,
    moe_ref,
    kv_v,
    wo_v,
    wg_v,
    wu_v,
    wd_v,
    qall,
    head_rows,
    pacc,
    pstat,
    abuf,
    hbuf,
    ssq,
    gacc,
    uacc,
    act,
    sbuf,
    rbuf,
    load_sem,
    wg_sem,
    wu_sem,
    wd_sem,
    q_sem,
    pacc_sem,
    pstat_sem,
    a_sem,
    h_sem,
    ssq_sem,
    r_sem,
):
    e = lax.axis_index("expert")
    t = lax.axis_index("tensor")
    own_seqs = q_ref.shape[0]
    seqs = own_seqs * experts_n
    heads = q_ref.shape[1] // HD
    kv_local = new_ref.shape[2] // HD
    group_size = heads // kv_local
    positions = kv_v.shape[1]
    keys2 = 2 * positions
    kv_flat = kv_v.reshape(kv_v.shape[0], keys2, kv_v.shape[3])
    cols = wo_v.shape[1]
    scale = 1.0 / math.sqrt(HD)
    f32 = jnp.float32
    bf16 = jnp.bfloat16

    kv_load = pltpu.make_async_copy(kv_hbm, kv_v, load_sem.at[1])
    kv_load.start()
    wo_load = pltpu.make_async_copy(wo_hbm, wo_v, load_sem.at[0])
    wo_load.start()

    def column_block(step, sign):
        return lax.rem(e + sign * step + experts_n, experts_n) * cols

    gate_loads, up_loads, down_loads = [], [], []
    for step in range(experts_n):
        rows = pl.ds(pl.multiple_of(column_block(step, -1), 128), cols)
        for hbm, vmem, sem, loads in (
            (wg_hbm, wg_v, wg_sem, gate_loads),
            (wu_hbm, wu_v, wu_sem, up_loads),
        ):
            load = pltpu.make_async_copy(hbm.at[0, rows, :], vmem.at[rows, :], sem.at[step])
            load.start()
            loads.append(load)
    down_order = list(range(1, experts_n)) + [0]
    for step in down_order:
        block = pl.ds(pl.multiple_of(column_block(step, 1), 128), cols)
        load = pltpu.make_async_copy(
            wd_hbm.at[0, :, block], wd_v.at[:, block], wd_sem.at[step]
        )
        load.start()
        down_loads.append(load)

    barrier = pltpu.get_barrier_semaphore()
    for k in range(1, experts_n * tensor_n):
        where = {
            "expert": lax.rem(e + k // tensor_n, experts_n),
            "tensor": lax.rem(t + k % tensor_n, tensor_n),
        }
        pl.semaphore_signal(barrier, inc=1, device_id=where, device_id_type=MESH)
    pl.semaphore_wait(barrier, experts_n * tensor_n - 1)

    sends = []
    q_copies = []
    for step in range(1, experts_n):
        copy = remote(
            q_ref, qall.at[e], q_sem, step, {"expert": lax.rem(e + step, experts_n)}
        )
        copy.start()
        q_copies.append(copy)
    qall[e] = q_ref[...]
    kv_load.wait()
    for copy in q_copies:
        copy.wait_recv()
    for owner in range(experts_n):
        block = qall[owner].astype(f32)
        for h in range(heads):
            head_rows[pl.ds(owner * own_seqs * heads + h, own_seqs, stride=heads), :] = block[
                :, h * HD : (h + 1) * HD
            ]

    row_of = lax.broadcasted_iota(jnp.int32, (heads, HD), 0)
    column = lax.broadcasted_iota(jnp.int32, (heads, keys2), 1)
    is_key = lax.rem(column, 2) == 0
    position = e * positions + lax.div(column, 2)

    def by_group(pieces):
        picked = pieces[0]
        for g in range(1, kv_local):
            picked = jnp.where(row_of >= g * group_size, pieces[g], picked)
        return picked

    cache_list, score_list, live_list, own_list, value_list = [], [], [], [], []
    for b in range(seqs):
        q_rows = head_rows[b * heads : (b + 1) * heads, :]
        spread = jnp.concatenate(
            [
                jnp.where(lax.div(row_of, group_size) == g, q_rows, 0.0)
                for g in range(kv_local)
            ],
            axis=1,
        ).astype(bf16)
        cache_list.append(kv_flat[slot_ref[b]])
        raw = lax.dot_general(
            spread, cache_list[b], (((1,), (1,)), ((), ())), preferred_element_type=f32
        )
        live = is_key & (position < len_ref[b])
        score_list.append(jnp.where(live, raw * scale, MASKED))
        live_list.append(jnp.where(live, 1.0, 0.0))
        fresh = new_ref[b % own_seqs].astype(f32)
        fresh_keys = by_group([fresh[0:1, g * HD : (g + 1) * HD] for g in range(kv_local)])
        own = jnp.sum(q_rows * fresh_keys, axis=1, keepdims=True) * scale
        own_list.append(jnp.where(e == b // own_seqs, own, MASKED))
        value_list.append(
            jnp.broadcast_to(
                by_group([fresh[1:2, g * HD : (g + 1) * HD] for g in range(kv_local)]),
                (heads, HD),
            )
        )
    scores = jnp.concatenate(score_list, axis=0)
    live = jnp.concatenate(live_list, axis=0)
    own = jnp.concatenate(own_list, axis=0)
    peak = jnp.maximum(jnp.max(scores, axis=1, keepdims=True), own)
    weights = jnp.exp(scores - peak) * live
    own_weight = jnp.where(own > 0.5 * MASKED, jnp.exp(own - peak), 0.0)
    total = jnp.sum(weights, axis=1, keepdims=True) + own_weight
    shifted = pltpu.roll(weights, 1, 1).astype(bf16)
    for b in range(seqs):
        out = jnp.dot(
            shifted[b * heads : (b + 1) * heads, :],
            cache_list[b],
            preferred_element_type=f32,
        )
        picked = by_group([out[:, g * HD : (g + 1) * HD] for g in range(kv_local)])
        picked = picked + own_weight[b * heads : (b + 1) * heads] * value_list[b]
        head_rows[b * heads : (b + 1) * heads, :] = picked
    pacc[0] = head_rows[...].astype(bf16)
    lane = lax.broadcasted_iota(jnp.int32, (seqs * heads, HD), 1)
    stats = jnp.where(lane == 0, peak, jnp.where(lane == 1, total, 0.0))
    pstat[0] = stats.T[0:2, :]

    p_copies = []
    for step in range(1, experts_n):
        where = {"expert": lax.rem(e + step, experts_n)}
        for buffer, sem in ((pstat, pstat_sem), (pacc, pacc_sem)):
            copy = remote(buffer.at[0], buffer.at[step], sem, step, where)
            copy.start()
            p_copies.append(copy)

    logits = logits_ref[...]
    first_share = 1.0 / (1.0 + jnp.exp(logits[1:2, :] - logits[0:1, :]))
    ids = ids_ref[...]
    mix_row = jnp.where(ids[0:1, :] == e, first_share, 0.0) + jnp.where(
        ids[1:2, :] == e, 1.0 - first_share, 0.0
    )
    diagonal = lax.broadcasted_iota(jnp.int32, (seqs, seqs), 0) == lax.broadcasted_iota(
        jnp.int32, (seqs, seqs), 1
    )
    mix = jnp.sum(jnp.where(diagonal, mix_row, 0.0), axis=1, keepdims=True)

    wo_load.wait()
    for copy in p_copies:
        copy.wait_recv()
    peaks = [pstat[j][0:1, :] for j in range(experts_n)]
    top = functools.reduce(jnp.maximum, peaks)
    factors = [jnp.exp(p - top) for p in peaks]
    whole = sum(f * pstat[j][1:2, :] for j, f in enumerate(factors))
    row8 = lax.broadcasted_iota(jnp.int32, (8, seqs * heads), 0)
    stacked = jnp.zeros((8, seqs * heads), f32)
    for j, f in enumerate(factors):
        stacked = jnp.where(row8 == j, f / whole, stacked)
    turned = stacked.T
    context = sum(pacc[j].astype(f32) * turned[:, j : j + 1] for j in range(experts_n))
    head_rows[...] = context
    context = jnp.concatenate(
        [head_rows[pl.ds(h, seqs, stride=heads), :] for h in range(heads)], axis=1
    ).astype(bf16)
    abuf[t] = jnp.dot(context, wo_v[...], preferred_element_type=f32).astype(bf16)

    a_copies = []
    for step in range(1, tensor_n):
        copy = remote(
            abuf.at[t], abuf.at[t], a_sem, step, {"tensor": lax.rem(t + step, tensor_n)}
        )
        copy.start()
        a_copies.append(copy)
    for copy in a_copies:
        copy.wait_recv()
    attention = sum(abuf[j].astype(f32) for j in range(tensor_n)).astype(bf16)
    attn_ref[...] = attention
    hidden = resid_ref[...].astype(f32) + attention.astype(f32)
    gain_rows = gain_ref[...].astype(f32)
    gain = jnp.concatenate([gain_rows[i : i + 1, :] for i in range(gain_rows.shape[0])], axis=1)
    hbuf[0] = (hidden * gain).astype(bf16)
    square_sums = jnp.sum(hidden * hidden, axis=1, keepdims=True)
    wide_diagonal = lax.broadcasted_iota(jnp.int32, (seqs, 128), 0) == lax.broadcasted_iota(
        jnp.int32, (seqs, 128), 1
    )
    ssq[0] = jnp.sum(jnp.where(wide_diagonal, square_sums, 0.0), axis=0, keepdims=True)
    h_copies, s_copies = [None], [None]
    for step in range(1, experts_n):
        where = {"expert": lax.rem(e + step, experts_n)}
        copy = remote(hbuf.at[0], hbuf.at[step], h_sem, step, where)
        copy.start()
        h_copies.append(copy)
        copy = remote(ssq.at[0], ssq.at[step], ssq_sem, step, where)
        copy.start()
        s_copies.append(copy)

    hidden_units = wg_v.shape[1]
    width = math.gcd(hidden_units, 512)
    for step in range(experts_n):
        if step:
            h_copies[step].wait_recv()
        gate_loads[step].wait()
        up_loads[step].wait()
        rows = pl.ds(pl.multiple_of(column_block(step, -1), 128), cols)
        tokens = hbuf[step]

        def one(i, carry, rows=rows, tokens=tokens, step=step):
            block = pl.ds(pl.multiple_of(i * width, width), width)
            gate = jnp.dot(tokens, wg_v[rows, block], preferred_element_type=f32)
            up = jnp.dot(tokens, wu_v[rows, block], preferred_element_type=f32)
            if step:
                gate = gate + gacc[:, block]
                up = up + uacc[:, block]
            gacc[:, block] = gate
            uacc[:, block] = up
            return carry

        lax.fori_loop(0, hidden_units // width, one, 0)
    for step in range(1, experts_n):
        s_copies[step].wait_recv()
    square_row = sum(ssq[j] for j in range(experts_n))
    squares = jnp.sum(jnp.where(wide_diagonal, square_row, 0.0), axis=1, keepdims=True)
    inverse = lax.rsqrt(squares / (cols * experts_n) + EPSILON)
    gate = gacc[...] * inverse
    up = uacc[...] * inverse
    act[...] = (gate / (1.0 + jnp.exp(-gate)) * up).astype(bf16)

    out_rows = seqs // tensor_n
    down_width = math.gcd(cols, 512)
    r_copies = []
    for step, load in zip(down_order, down_loads):
        load.wait()
        start = column_block(step, 1)

        def one_down(i, carry, start=start, step=step):
            offset = pl.multiple_of(i * down_width, down_width)
            block = pl.ds(pl.multiple_of(start + offset, 128), down_width)
            made = jnp.dot(act[...], wd_v[:, block], preferred_element_type=f32) * mix
            for p in range(tensor_n):
                sbuf[step, p, :, pl.ds(offset, down_width)] = made[
                    p * out_rows : (p + 1) * out_rows
                ].astype(bf16)
            return carry

        lax.fori_loop(0, cols // down_width, one_down, 0)
        for turn in range(tensor_n):
            if step == 0 and turn == 0:
                continue
            k = step * tensor_n + turn
            target = lax.rem(t + turn, tensor_n)
            where = {"expert": lax.rem(e + step, experts_n), "tensor": target}
            copy = remote(sbuf.at[step, target], rbuf.at[k], r_sem, k, where)
            copy.start()
            r_copies.append(copy)
    result = sbuf[0, t].astype(f32)
    for copy in r_copies:
        copy.wait_recv()
    for k in range(1, experts_n * tensor_n):
        result = result + rbuf[k].astype(f32)
    moe_ref[...] = result.astype(bf16)
    for copy in (
        q_copies + p_copies + a_copies + h_copies[1:] + s_copies[1:] + r_copies
    ):
        copy.wait_send()


def write_results(attention_ref, produced_ref, attn_ref, moe_ref):
    attn_ref[...] = attention_ref[...]
    moe_ref[...] = produced_ref[...]


def fused(
    kv_prefill, slot_of, lengths, query, new_kv, wo, resid, norm_gain, expert_ids,
    gate_logits, gate_weight_slabs, w_up, w_down,
):
    experts_n = lax.axis_size("expert")
    tensor_n = lax.axis_size("tensor")
    slots, positions, _, kv_cols = kv_prefill.shape
    own_seqs = query.shape[0]
    seqs = lengths.shape[0]
    cols = resid.shape[1]
    heads = query.shape[1] // HD
    hidden_units = w_down.shape[1]
    out_rows = seqs // tensor_n
    bf16 = jnp.bfloat16
    f32 = jnp.float32
    vmem = pl.BlockSpec(memory_space=pltpu.VMEM)
    smem = pl.BlockSpec(memory_space=pltpu.SMEM)
    hbm = pl.BlockSpec(memory_space=pl.ANY)
    dma = pltpu.SemaphoreType.DMA
    peers = experts_n * tensor_n
    attention, produced = (
        pl.pallas_call(
            functools.partial(fused_kernel, experts_n, tensor_n),
            out_shape=(
                jax.ShapeDtypeStruct((seqs, cols), bf16),
                jax.ShapeDtypeStruct((out_rows, cols), bf16),
            ),
            in_specs=[smem, smem] + [vmem] * 6 + [hbm] * 5,
            out_specs=(vmem, vmem),
            scratch_shapes=[
                pltpu.VMEM(kv_prefill.shape, bf16),
                pltpu.VMEM(wo.shape, bf16),
                pltpu.VMEM(gate_weight_slabs.shape[1:], bf16),
                pltpu.VMEM(w_up.shape[1:], bf16),
                pltpu.VMEM(w_down.shape[1:], bf16),
                pltpu.VMEM((experts_n,) + query.shape, bf16),
                pltpu.VMEM((seqs * heads, HD), f32),
                pltpu.VMEM((experts_n, seqs * heads, HD), bf16),
                pltpu.VMEM((experts_n, 2, seqs * heads), f32),
                pltpu.VMEM((tensor_n, seqs, cols), bf16),
                pltpu.VMEM((experts_n, seqs, cols), bf16),
                pltpu.VMEM((experts_n, 1, 128), f32),
                pltpu.VMEM((seqs, hidden_units), f32),
                pltpu.VMEM((seqs, hidden_units), f32),
                pltpu.VMEM((seqs, hidden_units), bf16),
                pltpu.VMEM((experts_n, tensor_n, out_rows, cols), bf16),
                pltpu.VMEM((peers, out_rows, cols), bf16),
                dma((2,)),
                dma((experts_n,)),
                dma((experts_n,)),
                dma((experts_n,)),
                dma((2, experts_n)),
                dma((2, experts_n)),
                dma((2, experts_n)),
                dma((2, tensor_n)),
                dma((2, experts_n)),
                dma((2, experts_n)),
                dma((2, peers)),
            ],
            compiler_params=pltpu.CompilerParams(
                collective_id=0, has_side_effects=True, vmem_limit_bytes=60 * 1024 * 1024
            ),
        )(
            slot_of, lengths, query, new_kv, resid, norm_gain.reshape(cols // 128, 128), expert_ids.T,
            gate_logits.T, kv_prefill, wo,
            gate_weight_slabs, w_up, w_down,
        )
    )

    return pl.pallas_call(
        write_results,
        out_shape=(
            jax.ShapeDtypeStruct(attention.shape, bf16),
            jax.ShapeDtypeStruct(produced.shape, bf16),
        ),
        in_specs=[vmem, vmem],
        out_specs=(vmem, vmem),
    )(attention, produced)


def layer(*arrays):
    kv_prefill, slot_of, lengths, query = arrays[:4]
    gate_slabs = arrays[10]
    weights = 3 * gate_slabs.size * 2
    rows = lengths.shape[0] * (query.shape[1] // HD)
    if (
        lax.axis_size("expert") == EXPERTS
        and gate_slabs.shape[0] == 1
        and (2 * kv_prefill.shape[1]) % 128 == 0
        and (query.shape[1] // HD) % 8 == 0
        and lengths.shape[0] % 16 == 0
        and rows == 128
        and weights <= 52 * 2**20
    ):
        return fused(*arrays)
    return shards(*arrays)


def solution(mesh):
    return jax.shard_map(
        layer,
        mesh=mesh,
        in_specs=(
            P("groups", "expert", None, "tensor"),
            P("groups"),
            P("groups"),
            P(("groups", "expert"), "tensor"),
            P(("groups", "expert"), None, "tensor"),
            P("tensor", "expert"),
            P("groups", "expert"),
            P("expert"),
            P("groups", None),
            P("groups", None),
            P("expert", None, "tensor"),
            P("expert", None, "tensor"),
            P("expert", "tensor", None),
        ),
        out_specs=(P("groups", "expert"), P(("groups", "tensor"), "expert")),
        check_vma=False,
    )
```
